32 devices in a mesh: rows: 8 (over z, x), width: 4 (over y, core).
Axes of the slice: x: 2, y: 2, z: 4, core: 2. Of those that a mesh axis runs over, the one named last changes fastest.
Arguments:
- weight_gate: float32 [2560, 9728], P('rows', 'width'), may hold values from -0.15625 to 0.15625
- moment_gate: float32 [2560, 9728], P('rows', 'width'), may hold values from -6 to 6
- square_gate: float32 [2560, 9728], P('rows', 'width'), may hold values from 0.1 to 10
- weight_up: float32 [2560, 9728], P('rows', 'width'), may hold values from -0.15625 to 0.15625
- moment_up: float32 [2560, 9728], P('rows', 'width'), may hold values from -6 to 6
- square_up: float32 [2560, 9728], P('rows', 'width'), may hold values from 0.1 to 10
- norm_gain: float32 [2560], P('rows'), may hold values from 0.25 to 1.75
Outputs:
- ready_gate: bfloat16 [2560, 9728], P(None, 'width')
- ready_up: bfloat16 [2560, 9728], P(None, 'width')
- column_gate: float32 [9728], P('width')
- column_up: float32 [9728], P('width')
The draws below stay inside these ranges and needn't reach their ends.
All inputs are finite; a program needn't handle non-finite values.
Results may differ from the reference program's by a relative error of at most 0.0004.
Values may be sent and summed in bfloat16 or wider, within the bound.
A program may use at most 128 MiB of HBM per device.

```python
import math
import jax
import jax.numpy as jnp
from jax import lax

D_MODEL = 2560
D_INNER = 9728


def with_spikes(values, rng, source, target, blocks, factor):
    def block_of(axis_at):
        return (jnp.arange(values.shape[axis_at]) // (values.shape[axis_at] // blocks)).reshape((-1,) + (1,) * (values.ndim - 1 - axis_at))

    one_side = jax.random.permutation(rng, blocks)[block_of(target)]
    second = (block_of(target) + blocks // 2) % blocks
    return jnp.where((block_of(source) == one_side) | (block_of(source) == second), factor * values, values)


def block_levels(rng, extent, pieces, smallest, top_value):
    loudness, own = 1.0, jax.random.fold_in(rng, 6)
    for dim, blocks in pieces:
        heights = jnp.exp(jax.random.uniform(jax.random.fold_in(own, dim), (blocks,), jnp.float32, smallest / len(pieces), top_value / len(pieces)))
        loudness = loudness * jnp.repeat(heights, extent[dim] // blocks).reshape([-1 if axis == dim else 1 for axis in range(len(extent))])
    return loudness


def normal_values(own_key, shape, scale, limit, split=(), held_as=jnp.bfloat16):
    array = scale * jax.random.normal(own_key, shape, jnp.float32)
    if split:
        array = array * block_levels(own_key, shape, split, -0.22, 0.18)
    return jnp.clip(array, -limit, limit).astype(held_as)


def noise_with(rng, dims, spread, most, shards, heavy, dtype=jnp.bfloat16):
    entries = spread * jax.random.normal(rng, dims, jnp.float32)
    if shards:
        entries = entries * block_levels(rng, dims, shards, -0.22, 0.18)
    return jnp.clip(with_spikes(entries, jax.random.fold_in(rng, 3), *heavy), -most, most).astype(dtype)


def setup_inputs(seed: int = 0) -> dict:
    arg_keys = jax.random.split(jax.random.key(seed), 8)
    return {
        "weight_gate": noise_with(arg_keys[0], (D_MODEL, D_INNER), D_MODEL ** -0.5, 0.15625, ((0, 8), (1, 4)), (0, 1, 8, 2.0), jnp.float32),
        "moment_gate": normal_values(arg_keys[1], (D_MODEL, D_INNER), 1.0, 6.0, ((0, 8), (1, 4)), jnp.float32),
        "square_gate": jnp.clip(jnp.exp(math.log(10.0) - 4.6051702 * jax.random.uniform(arg_keys[2], (D_MODEL, D_INNER), jnp.float32) ** block_levels(arg_keys[2], (D_MODEL, D_INNER), ((0, 8), (1, 4)), -0.2, 0.2)), 0.1, 10.0),
        "weight_up": noise_with(arg_keys[3], (D_MODEL, D_INNER), D_MODEL ** -0.5, 0.15625, ((0, 8), (1, 4)), (0, 1, 8, 2.0), jnp.float32),
        "moment_up": normal_values(arg_keys[4], (D_MODEL, D_INNER), 1.0, 6.0, ((0, 8), (1, 4)), jnp.float32),
        "square_up": jnp.clip(jnp.exp(math.log(10.0) - 4.6051702 * jax.random.uniform(arg_keys[5], (D_MODEL, D_INNER), jnp.float32) ** block_levels(arg_keys[5], (D_MODEL, D_INNER), ((0, 8), (1, 4)), -0.2, 0.2)), 0.1, 10.0),
        "norm_gain": jnp.clip(1.0 + 0.15 * jax.random.normal(arg_keys[6], (D_MODEL,), jnp.float32), 0.25, 1.75),
    }


learn_rate = 0.02
decay_rate = 0.1
tiny_value = 1e-08

def reference(weight_gate, moment_gate, square_gate, weight_up, moment_up, square_up, norm_gain):
    latest_gate = weight_gate - learn_rate * (moment_gate / (jnp.sqrt(square_gate) + tiny_value) + decay_rate * weight_gate)
    latest_up = weight_up - learn_rate * (moment_up / (jnp.sqrt(square_up) + tiny_value) + decay_rate * weight_up)
    latest_gained_gate = latest_gate * norm_gain[:, None]
    latest_gained_up = latest_up * norm_gain[:, None]
    column_gate = jnp.sqrt(lax.optimization_barrier(jnp.sum(latest_gained_gate * latest_gained_gate, axis=0)))
    ready_gate = (latest_gained_gate / column_gate).astype(jnp.bfloat16)
    column_up = jnp.sqrt(lax.optimization_barrier(jnp.sum(latest_gained_up * latest_gained_up, axis=0)))
    ready_up = (latest_gained_up / column_up).astype(jnp.bfloat16)
    return (ready_gate, ready_up, column_gate, column_up)
```

```python
import functools

import jax
import jax.numpy as jnp
from jax import lax
from jax.experimental import pallas as pl
from jax.experimental.pallas import tpu as pltpu
from jax.sharding import PartitionSpec as P

learn_rate = 0.02
decay_rate = 0.1
tiny_value = 1e-08
lanes = 128
vmem_bytes = 67043328
block_rows = 16
MESH = pl.DeviceIdType.MESH
scope = jax.named_scope


def column_cuts(columns):
    tiles = columns // lanes
    first = max(1, tiles // 9)
    rest = tiles - first
    sizes = [first] + [rest // 3 + (1 if i < rest % 3 else 0) for i in range(3)]
    cuts, at = [], 0
    for size in sizes:
        if size:
            cuts.append((at * lanes, size * lanes))
        at += size
    return cuts


def gather_kernel(
    n, gain_ref, wg, mg, sg, wu, mu, su, out_gate, out_up, col_gate, col_up,
    held, gain_row, gain_wide, parts,
    gain_sem, in_sem, part_send, part_recv, send_sem, line_recv, mate_recv, rest_recv,
):
    me = lax.axis_index("rows")
    w = lax.axis_index("width")
    length = n // 2
    place, side = me // 2, me % 2
    mate = place + 1 - 2 * (place % 2)
    rows, columns = wg.shape
    cuts = column_cuts(columns)
    half = len(cuts)
    chunks = [(t, at, size) for t in range(2) for at, size in cuts]
    sources = ((wg, mg, sg), (wu, mu, su))
    outs = (out_gate, out_up)
    cols = (col_gate, col_up)

    barrier = pltpu.get_barrier_semaphore()

    def greet(i, carry):
        peer = lax.rem(me + i, n)
        pl.semaphore_signal(barrier, inc=1, device_id=(peer, w), device_id_type=MESH)
        return carry

    lax.fori_loop(1, n, greet, 0)

    def fetch(k):
        t, at, size = chunks[k]
        for i, src in enumerate(sources[t]):
            pltpu.make_async_copy(
                src.at[:, pl.ds(at, size)], held.at[i, t, :, pl.ds(at, size)], in_sem.at[k]
            ).start()

    def fetched(k):
        t, at, size = chunks[k]
        here = held.at[:, t, :, pl.ds(at, size)]
        pltpu.make_async_copy(here, here, in_sem.at[k]).wait()

    gain_copy = pltpu.make_async_copy(gain_ref, gain_row.at[0], gain_sem)
    gain_copy.start()
    fetch(0)
    fetch(1)
    with scope("gain"):
        gain_copy.wait()
    for r in range(0, rows, 8):
        at = r // lanes * lanes
        wide = min(lanes, rows - at)
        row = jnp.broadcast_to(gain_row[:, pl.ds(at, wide)], (8, wide))
        lane = lax.broadcasted_iota(jnp.int32, (8, wide), 1)
        here = lax.broadcasted_iota(jnp.int32, (8, wide), 0) + (r - at)
        picked = jnp.sum(jnp.where(lane == here, row, 0.0), axis=1, keepdims=True)
        gain_wide[pl.ds(r, 8), :] = jnp.broadcast_to(picked, (8, lanes))

    def part_copy(k, peer):
        t, at, size = chunks[k]
        here = parts.at[me, t, :, pl.ds(at, size)]
        return pltpu.make_async_remote_copy(
            src_ref=here, dst_ref=here, send_sem=part_send, recv_sem=part_recv.at[k],
            device_id=(peer, w), device_id_type=MESH,
        )

    def compute(k):
        t, at, size = chunks[k]
        with scope(f"fetched{k}"):
            fetched(k)

        def step(b, total):
            here = pl.ds(pl.multiple_of(b * block_rows, block_rows), block_rows)
            there = pl.ds(at, size)
            weight = held[0, t, here, there]
            latest = weight - learn_rate * (
                held[1, t, here, there] / (jnp.sqrt(held[2, t, here, there]) + tiny_value) + decay_rate * weight
            )
            gain = jnp.concatenate([gain_wide[here, :]] * (size // lanes), axis=1)
            gained = latest * gain
            held[0, t, here, there] = gained
            squared = gained * gained
            for r in range(0, block_rows, 8):
                total = total + squared[r : r + 8]
            return total

        total = lax.fori_loop(0, rows // block_rows, step, jnp.zeros((8, size), jnp.float32))
        parts[me, t, :, pl.ds(at, size)] = jnp.sum(total, axis=0, keepdims=True)

    def share_parts(k):
        def send(i, carry):
            part_copy(k, lax.rem(me + i, n)).start()
            return carry

        lax.fori_loop(1, n, send, 0)

    def parts_arrived(k):
        t, at, size = chunks[k]
        refs = parts.at[pl.ds(0, n - 1), t, :, pl.ds(at, size)]
        pltpu.make_async_copy(refs, refs, part_recv.at[k]).wait()

    def block(share, k):
        t, at, size = chunks[k]
        start = pl.multiple_of(share * rows, rows)
        return outs[t].at[pl.ds(start, rows), pl.ds(at, size)]

    def push(link, share, k, recv):
        there = ((place - 1) * 2 + side, (place + 1) * 2 + side, place * 2 + 1 - side)[link]
        here = block(share, k)
        pltpu.make_async_remote_copy(
            src_ref=here, dst_ref=here, send_sem=send_sem.at[link, chunks[k][0]], recv_sem=recv,
            device_id=(there, w), device_id_type=MESH,
        ).start()

    def arrived(share, k, recv):
        here = block(share, k)
        pltpu.make_async_copy(here, here, recv).wait()

    def push_line(link, q, k):
        push(link, q * 2 + side, k, line_recv.at[q, k])

    def push_side(q, k, own=False):
        share = q * 2 + side
        if k < half:
            push(2, share, k, rest_recv.at[0])
        elif own:
            push(2, share, k, mate_recv.at[k - half])
        else:
            @pl.when(q != mate)
            def _():
                push(2, share, k, rest_recv.at[1])

    def finish(k):
        t, at, size = chunks[k]
        with scope(f"parts{k}"):
            parts_arrived(k)
        total = parts[0, t, :, pl.ds(at, size)]
        for i in range(1, n):
            total = total + parts[i, t, :, pl.ds(at, size)]
        scale = jnp.sqrt(total)
        cols[t][:, pl.ds(at, size)] = scale

        def step(b, carry):
            here = pl.ds(pl.multiple_of(b * block_rows, block_rows), block_rows)
            there = pl.ds(pl.multiple_of(me * rows + b * block_rows, block_rows), block_rows)
            outs[t][there, pl.ds(at, size)] = (held[0, t, here, pl.ds(at, size)] / scale).astype(jnp.bfloat16)
            return carry

        lax.fori_loop(0, rows // block_rows, step, 0)

    def send_own(k):
        @pl.when(place > 0)
        def _():
            push_line(0, place, k)

        @pl.when(place < length - 1)
        def _():
            push_line(1, place, k)

        push_side(place, k, own=True)

    for k in range(2, len(chunks)):
        fetch(k)
    compute(0)
    with scope("barrier"):
        pl.semaphore_wait(barrier, n - 1)
    share_parts(0)
    for k in range(len(chunks)):
        if k + 1 < len(chunks):
            compute(k + 1)
            share_parts(k + 1)
        finish(k)
        with scope(f"own{k}"):
            send_own(k)

    def spread(d, carry):
        for k in range(len(chunks)):
            @pl.when(place + d < length)
            def _():
                q = place + d
                with scope(f"R{k}"):
                    arrived(q * 2 + side, k, line_recv.at[q, k])

                @pl.when(place > 0)
                def _():
                    push_line(0, q, k)

                push_side(q, k)

            @pl.when(place - d >= 0)
            def _():
                q = place - d
                with scope(f"L{k}"):
                    arrived(q * 2 + side, k, line_recv.at[q, k])

                @pl.when(place < length - 1)
                def _():
                    push_line(1, q, k)

                push_side(q, k)

        return carry

    middle = max(1, length // 2) + 1
    lax.fori_loop(1, middle, spread, 0)

    other = place * 2 + 1 - side
    for k in range(half, len(chunks)):
        with scope(f"X{k}"):
            arrived(other, k, mate_recv.at[k - half])

        @pl.when(mate < place)
        def _():
            push(0, other, k, rest_recv.at[2])

        @pl.when(mate > place)
        def _():
            push(1, other, k, rest_recv.at[2])

    lax.fori_loop(middle, length, spread, 0)

    def pass_bytes(t, shares, sem):
        here = outs[t].at[pl.ds(0, shares * rows)]
        pltpu.make_async_copy(here, here, sem).wait()

    with scope("rest"):
        pass_bytes(0, length, rest_recv.at[0])
        if length > 2:
            pass_bytes(1, length - 2, rest_recv.at[1])
        pass_bytes(1, 1, rest_recv.at[2])

    with scope("drain"):
        everyone = parts.at[pl.ds(0, n - 1)]
        pltpu.make_async_copy(everyone, everyone, part_send).wait()
        pass_bytes(0, length, send_sem.at[2, 0])
        pass_bytes(1, length - 1, send_sem.at[2, 1])
        for p in range(length):
            @pl.when(place == p)
            def _():
                if p > 0:
                    pass_bytes(0, length - p, send_sem.at[0, 0])
                    pass_bytes(1, length - p + p % 2, send_sem.at[0, 1])
                if p < length - 1:
                    pass_bytes(0, p + 1, send_sem.at[1, 0])
                    pass_bytes(1, p + 1 + 1 - p % 2, send_sem.at[1, 1])


def write_kernel(pieces, gate, up, col_gate, col_up, out_gate, out_up, out_col_gate, out_col_up, sem):
    step = gate.shape[0] // pieces
    for i in range(pieces):
        for t, (src, dst) in enumerate(((gate, out_gate), (up, out_up))):
            pltpu.make_async_copy(src.at[pl.ds(i * step, step)], dst.at[pl.ds(i * step, step)], sem.at[t]).start()
    small = [
        pltpu.make_async_copy(src.at[0], dst, sem.at[2 + t])
        for t, (src, dst) in enumerate(((col_gate, out_col_gate), (col_up, out_col_up)))
    ]
    for copy in small:
        copy.start()
    for t, (src, dst) in enumerate(((gate, out_gate), (up, out_up))):
        pltpu.make_async_copy(src, dst, sem.at[t]).wait()
    for copy in small:
        copy.wait()


def write_out(pieces, gate, up, col_gate, col_up):
    vmem = pl.BlockSpec(memory_space=pltpu.VMEM)
    hbm = pl.BlockSpec(memory_space=pltpu.HBM)
    flat = jax.ShapeDtypeStruct((col_gate.shape[1],), col_gate.dtype)
    return pl.pallas_call(
        functools.partial(write_kernel, pieces),
        out_shape=[jax.ShapeDtypeStruct(a.shape, a.dtype) for a in (gate, up)] + [flat, flat],
        in_specs=[vmem] * 4,
        out_specs=[hbm] * 4,
        scratch_shapes=[pltpu.SemaphoreType.DMA((4,))],
        compiler_params=pltpu.CompilerParams(vmem_limit_bytes=2**20),
        name="write_out",
    )(gate, up, col_gate, col_up)


def per_device(n, weight_gate, moment_gate, square_gate, weight_up, moment_up, square_up, norm_gain):
    rows, columns = weight_gate.shape
    half = len(column_cuts(columns))
    count = 2 * half
    vmem = pl.BlockSpec(memory_space=pltpu.VMEM)
    hbm = pl.BlockSpec(memory_space=pltpu.HBM)
    room = vmem_bytes - 2 * n * rows * columns * 2 - 3 * 2**19
    ready_gate, ready_up, column_gate, column_up = pl.pallas_call(
        functools.partial(gather_kernel, n),
        out_shape=(
            pltpu.VMEM((n * rows, columns), jnp.bfloat16),
            pltpu.VMEM((n * rows, columns), jnp.bfloat16),
            pltpu.VMEM((1, columns), jnp.float32),
            pltpu.VMEM((1, columns), jnp.float32),
        ),
        in_specs=[hbm] * 7,
        out_specs=(vmem, vmem, vmem, vmem),
        scratch_shapes=[
            pltpu.VMEM((3, 2, rows, columns), jnp.float32),
            pltpu.VMEM((1, rows), jnp.float32),
            pltpu.VMEM((rows, lanes), jnp.float32),
            pltpu.VMEM((n, 2, 1, columns), jnp.float32),
            pltpu.SemaphoreType.DMA,
            pltpu.SemaphoreType.DMA((count,)),
            pltpu.SemaphoreType.DMA,
            pltpu.SemaphoreType.DMA((count,)),
            pltpu.SemaphoreType.DMA((3, 2)),
            pltpu.SemaphoreType.DMA((n // 2, count)),
            pltpu.SemaphoreType.DMA((half,)),
            pltpu.SemaphoreType.DMA((3,)),
        ],
        compiler_params=pltpu.CompilerParams(
            collective_id=0, has_side_effects=True, vmem_limit_bytes=room
        ),
        name="step_and_gather",
    )(norm_gain, weight_gate, moment_gate, square_gate, weight_up, moment_up, square_up)
    return write_out(n, ready_gate, ready_up, column_gate, column_up)


def solution(mesh):
    split = P("rows", "width")
    return jax.shard_map(
        functools.partial(per_device, mesh.shape["rows"]),
        mesh=mesh,
        in_specs=(split,) * 6 + (P("rows"),),
        out_specs=(P(None, "width"), P(None, "width"), P("width"), P("width")),
        check_vma=False,
    )
```

```python
import functools

import jax
import jax.numpy as jnp
from jax import lax
from jax.experimental import pallas as pl
from jax.experimental.pallas import tpu as pltpu
from jax.sharding import PartitionSpec as P

learn_rate = 0.02
decay_rate = 0.1
tiny_value = 1e-08
lanes = 128
vmem_bytes = 67043328
block_rows = 16
MESH = pl.DeviceIdType.MESH
scope = jax.named_scope


def column_chunks(columns):
    tiles = columns // lanes
    first, last = max(1, tiles // 9), max(1, (tiles + 1) // 4)
    chunks = []
    for t, sizes in enumerate(([first] + thirds(tiles - first), thirds(tiles - last) + [last])):
        at = 0
        for size in sizes:
            if size:
                chunks.append((t, at * lanes, size * lanes))
            at += size
    return chunks


def thirds(tiles):
    return [tiles // 3 + (1 if i < tiles % 3 else 0) for i in range(3)]


def gather_kernel(
    n, gain_ref, wg, mg, sg, wu, mu, su, out_gate, out_up, col_gate, col_up, tail_line, tail_side,
    held, gain_row, gain_wide, parts,
    gain_sem, in_sem, part_send, part_recv, send_sem, line_recv, mate_recv, rest_recv, tail_sem,
):
    me = lax.axis_index("rows")
    w = lax.axis_index("width")
    length = n // 2
    place, side = me // 2, me % 2
    mate = place + 1 - 2 * (place % 2)
    far = jnp.where(place * 2 < length, length - 1, 0)
    rows, columns = wg.shape
    chunks = column_chunks(columns)
    half = sum(t == 0 for t, _, _ in chunks)
    last = len(chunks) - 1
    body = chunks[last][1]
    sources = ((wg, mg, sg), (wu, mu, su))
    outs = (out_gate, out_up)
    cols = (col_gate, col_up)

    barrier = pltpu.get_barrier_semaphore()

    def greet(i, carry):
        peer = lax.rem(me + i, n)
        pl.semaphore_signal(barrier, inc=1, device_id=(peer, w), device_id_type=MESH)
        return carry

    lax.fori_loop(1, n, greet, 0)

    def fetch(k):
        t, at, size = chunks[k]
        for i, src in enumerate(sources[t]):
            pltpu.make_async_copy(
                src.at[:, pl.ds(at, size)], held.at[i, t, :, pl.ds(at, size)], in_sem.at[k]
            ).start()

    def fetched(k):
        t, at, size = chunks[k]
        here = held.at[:, t, :, pl.ds(at, size)]
        pltpu.make_async_copy(here, here, in_sem.at[k]).wait()

    gain_copy = pltpu.make_async_copy(gain_ref, gain_row.at[0], gain_sem)
    gain_copy.start()
    fetch(0)
    fetch(1)
    with scope("gain"):
        gain_copy.wait()
    for r in range(0, rows, 8):
        at = r // lanes * lanes
        wide = min(lanes, rows - at)
        row = jnp.broadcast_to(gain_row[:, pl.ds(at, wide)], (8, wide))
        lane = lax.broadcasted_iota(jnp.int32, (8, wide), 1)
        here = lax.broadcasted_iota(jnp.int32, (8, wide), 0) + (r - at)
        picked = jnp.sum(jnp.where(lane == here, row, 0.0), axis=1, keepdims=True)
        gain_wide[pl.ds(r, 8), :] = jnp.broadcast_to(picked, (8, lanes))

    def part_copy(k, peer):
        t, at, size = chunks[k]
        here = parts.at[me, t, :, pl.ds(at, size)]
        return pltpu.make_async_remote_copy(
            src_ref=here, dst_ref=here, send_sem=part_send, recv_sem=part_recv.at[k],
            device_id=(peer, w), device_id_type=MESH,
        )

    def compute(k):
        t, at, size = chunks[k]
        with scope(f"fetched{k}"):
            fetched(k)

        def step(b, total):
            here = pl.ds(pl.multiple_of(b * block_rows, block_rows), block_rows)
            there = pl.ds(at, size)
            weight = held[0, t, here, there]
            latest = weight - learn_rate * (
                held[1, t, here, there] / (jnp.sqrt(held[2, t, here, there]) + tiny_value) + decay_rate * weight
            )
            gain = jnp.concatenate([gain_wide[here, :]] * (size // lanes), axis=1)
            gained = latest * gain
            held[0, t, here, there] = gained
            squared = gained * gained
            for r in range(0, block_rows, 8):
                total = total + squared[r : r + 8]
            return total

        total = lax.fori_loop(0, rows // block_rows, step, jnp.zeros((8, size), jnp.float32))
        parts[me, t, :, pl.ds(at, size)] = jnp.sum(total, axis=0, keepdims=True)

    def share_parts(k):
        def send(i, carry):
            part_copy(k, lax.rem(me + i, n)).start()
            return carry

        lax.fori_loop(1, n, send, 0)

    def parts_arrived(k):
        t, at, size = chunks[k]
        refs = parts.at[pl.ds(0, n - 1), t, :, pl.ds(at, size)]
        pltpu.make_async_copy(refs, refs, part_recv.at[k]).wait()

    def block(share, k):
        t, at, size = chunks[k]
        start = pl.multiple_of(share * rows, rows)
        return outs[t].at[pl.ds(start, rows), pl.ds(at, size)]

    def push(link, share, k, recv, send):
        there = ((place - 1) * 2 + side, (place + 1) * 2 + side, place * 2 + 1 - side)[link]
        here = block(share, k)
        pltpu.make_async_remote_copy(
            src_ref=here, dst_ref=here, send_sem=send_sem.at[send], recv_sem=recv,
            device_id=(there, w), device_id_type=MESH,
        ).start()

    def arrived(share, k, recv):
        here = block(share, k)
        pltpu.make_async_copy(here, here, recv).wait()

    def push_line(link, q, k):
        push(link, q * 2 + side, k, line_recv.at[q, k], link * 2 + chunks[k][0])

    def push_side(q, k, own=False):
        share = q * 2 + side
        if k < half:
            push(2, share, k, rest_recv.at[0], 4)
        elif own:
            push(2, share, k, mate_recv.at[k - half], 6 if k == last else 5)
        elif k < last:
            @pl.when(q != mate)
            def _():
                push(2, share, k, rest_recv.at[1], 5)
        else:
            @pl.when((q != mate) & (q != far))
            def _():
                push(2, share, k, rest_recv.at[3], 6)

    def finish(k):
        t, at, size = chunks[k]
        with scope(f"parts{k}"):
            parts_arrived(k)
        total = parts[0, t, :, pl.ds(at, size)]
        for i in range(1, n):
            total = total + parts[i, t, :, pl.ds(at, size)]
        scale = jnp.sqrt(total)
        cols[t][:, pl.ds(at, size)] = scale

        def step(b, carry):
            here = pl.ds(pl.multiple_of(b * block_rows, block_rows), block_rows)
            there = pl.ds(pl.multiple_of(me * rows + b * block_rows, block_rows), block_rows)
            outs[t][there, pl.ds(at, size)] = (held[0, t, here, pl.ds(at, size)] / scale).astype(jnp.bfloat16)
            return carry

        lax.fori_loop(0, rows // block_rows, step, 0)

    def send_own(k):
        @pl.when(place > 0)
        def _():
            push_line(0, place, k)

        @pl.when(place < length - 1)
        def _():
            push_line(1, place, k)

        push_side(place, k, own=True)

    for k in range(2, len(chunks)):
        fetch(k)
    compute(0)
    with scope("barrier"):
        pl.semaphore_wait(barrier, n - 1)
    share_parts(0)
    for k in range(len(chunks)):
        if k + 1 < len(chunks):
            compute(k + 1)
            share_parts(k + 1)
        finish(k)
        with scope(f"own{k}"):
            send_own(k)

    def spread(d, carry):
        for k in range(len(chunks)):
            @pl.when(place + d < length)
            def _():
                q = place + d
                with scope(f"R{k}"):
                    arrived(q * 2 + side, k, line_recv.at[q, k])

                @pl.when(place > 0)
                def _():
                    push_line(0, q, k)

                push_side(q, k)

            @pl.when(place - d >= 0)
            def _():
                q = place - d
                with scope(f"L{k}"):
                    arrived(q * 2 + side, k, line_recv.at[q, k])

                @pl.when(place < length - 1)
                def _():
                    push_line(1, q, k)

                push_side(q, k)

        return carry

    middle = max(1, length // 2) + 1
    lax.fori_loop(1, middle, spread, 0)

    other = place * 2 + 1 - side
    for k in range(half, len(chunks)):
        with scope(f"X{k}"):
            arrived(other, k, mate_recv.at[k - half])
        if k < last:
            @pl.when(mate < place)
            def _():
                push(0, other, k, rest_recv.at[2], 7)

            @pl.when(mate > place)
            def _():
                push(1, other, k, rest_recv.at[2], 7)

    line_copy = pltpu.make_async_copy(block(other, last), tail_line, tail_sem.at[0])
    line_copy.start()
    lax.fori_loop(middle, length, spread, 0)
    side_copy = pltpu.make_async_copy(block(far * 2 + side, last), tail_side, tail_sem.at[1])
    side_copy.start()

    def pass_bytes(t, shares, sem, at=0, size=columns):
        here = outs[t].at[pl.ds(0, shares * rows), pl.ds(at, size)]
        pltpu.make_async_copy(here, here, sem).wait()

    with scope("rest"):
        pass_bytes(0, length, rest_recv.at[0])
        pass_bytes(1, length - 2, rest_recv.at[1], 0, body)
        pass_bytes(1, 1, rest_recv.at[2], 0, body)
        pass_bytes(1, length - 3, rest_recv.at[3], body, columns - body)

    with scope("drain"):
        everyone = parts.at[pl.ds(0, n - 1)]
        pltpu.make_async_copy(everyone, everyone, part_send).wait()
        pass_bytes(0, length, send_sem.at[4])
        pass_bytes(1, length - 1, send_sem.at[5], 0, body)
        pass_bytes(1, length - 2, send_sem.at[6], body, columns - body)
        pass_bytes(1, 1, send_sem.at[7], 0, body)
        for p in range(length):
            @pl.when(place == p)
            def _():
                for t in range(2):
                    if p > 0:
                        pass_bytes(t, length - p, send_sem.at[t])
                    if p < length - 1:
                        pass_bytes(t, p + 1, send_sem.at[2 + t])
        line_copy.wait()
        side_copy.wait()


def write_kernel(pieces, gate, up, col_gate, col_up, out_gate, out_up, out_col_gate, out_col_up, sem):
    step = gate.shape[0] // pieces
    for i in range(pieces):
        for t, (src, dst) in enumerate(((gate, out_gate), (up, out_up))):
            pltpu.make_async_copy(src.at[pl.ds(i * step, step)], dst.at[pl.ds(i * step, step)], sem.at[t]).start()
    small = [
        pltpu.make_async_copy(src.at[0], dst, sem.at[2 + t])
        for t, (src, dst) in enumerate(((col_gate, out_col_gate), (col_up, out_col_up)))
    ]
    for copy in small:
        copy.start()
    for t, (src, dst) in enumerate(((gate, out_gate), (up, out_up))):
        pltpu.make_async_copy(src, dst, sem.at[t]).wait()
    for copy in small:
        copy.wait()


def write_out(pieces, gate, up, col_gate, col_up):
    vmem = pl.BlockSpec(memory_space=pltpu.VMEM)
    hbm = pl.BlockSpec(memory_space=pltpu.HBM)
    flat = jax.ShapeDtypeStruct((col_gate.shape[1],), col_gate.dtype)
    return pl.pallas_call(
        functools.partial(write_kernel, pieces),
        out_shape=[jax.ShapeDtypeStruct(a.shape, a.dtype) for a in (gate, up)] + [flat, flat],
        in_specs=[vmem] * 4,
        out_specs=[hbm] * 4,
        scratch_shapes=[pltpu.SemaphoreType.DMA((4,))],
        compiler_params=pltpu.CompilerParams(vmem_limit_bytes=2**20),
        cost_estimate=pl.CostEstimate(flops=10**8, bytes_accessed=4 * gate.size, transcendentals=0),
        name="write_out",
    )(gate, up, col_gate, col_up)


def place_kernel(n, up, from_line, from_side, out, sem):
    me = lax.axis_index("rows")
    place, side = me // 2, me % 2
    mate = place + 1 - 2 * (place % 2)
    far = jnp.where(place * 2 < n // 2, n // 2 - 1, 0)
    rows, tail = from_line.shape
    copies = []
    for i, (src, q) in enumerate(((from_line, mate), (from_side, far))):
        start = pl.multiple_of((q * 2 + 1 - side) * rows, rows)
        there = out.at[pl.ds(start, rows), pl.ds(out.shape[1] - tail, tail)]
        copies.append(pltpu.make_async_copy(src, there, sem.at[i]))
    for copy in copies:
        copy.start()
    for copy in copies:
        copy.wait()


def place_tails(n, up, from_line, from_side):
    vmem = pl.BlockSpec(memory_space=pltpu.VMEM)
    hbm = pl.BlockSpec(memory_space=pltpu.HBM)
    return pl.pallas_call(
        functools.partial(place_kernel, n),
        out_shape=jax.ShapeDtypeStruct(up.shape, up.dtype),
        in_specs=[hbm, vmem, vmem],
        out_specs=hbm,
        input_output_aliases={0: 0},
        scratch_shapes=[pltpu.SemaphoreType.DMA((2,))],
        compiler_params=pltpu.CompilerParams(vmem_limit_bytes=2**20),
        name="place_tails",
    )(up, from_line, from_side)


def per_device(n, weight_gate, moment_gate, square_gate, weight_up, moment_up, square_up, norm_gain):
    rows, columns = weight_gate.shape
    length = n // 2
    chunks = column_chunks(columns)
    count, tail = len(chunks), chunks[-1][2]
    up_count = sum(t for t, _, _ in chunks)
    vmem = pl.BlockSpec(memory_space=pltpu.VMEM)
    hbm = pl.BlockSpec(memory_space=pltpu.HBM)
    room = vmem_bytes - 2 * n * rows * columns * 2 - 3 * 2**19
    ready_gate, ready_up, column_gate, column_up, tail_line, tail_side = pl.pallas_call(
        functools.partial(gather_kernel, n),
        out_shape=(
            pltpu.VMEM((n * rows, columns), jnp.bfloat16),
            pltpu.VMEM((n * rows, columns), jnp.bfloat16),
            pltpu.VMEM((1, columns), jnp.float32),
            pltpu.VMEM((1, columns), jnp.float32),
            jax.ShapeDtypeStruct((rows, tail), jnp.bfloat16),
            jax.ShapeDtypeStruct((rows, tail), jnp.bfloat16),
        ),
        in_specs=[hbm] * 7,
        out_specs=(vmem, vmem, vmem, vmem, hbm, hbm),
        scratch_shapes=[
            pltpu.VMEM((3, 2, rows, columns), jnp.float32),
            pltpu.VMEM((1, rows), jnp.float32),
            pltpu.VMEM((rows, lanes), jnp.float32),
            pltpu.VMEM((n, 2, 1, columns), jnp.float32),
            pltpu.SemaphoreType.DMA,
            pltpu.SemaphoreType.DMA((count,)),
            pltpu.SemaphoreType.DMA,
            pltpu.SemaphoreType.DMA((count,)),
            pltpu.SemaphoreType.DMA((8,)),
            pltpu.SemaphoreType.DMA((length, count)),
            pltpu.SemaphoreType.DMA((up_count,)),
            pltpu.SemaphoreType.DMA((4,)),
            pltpu.SemaphoreType.DMA((2,)),
        ],
        compiler_params=pltpu.CompilerParams(
            collective_id=0, has_side_effects=True, vmem_limit_bytes=room
        ),
        name="step_and_gather",
    )(norm_gain, weight_gate, moment_gate, square_gate, weight_up, moment_up, square_up)
    swap_line = [(i, (i // 2 ^ 1) * 2 + i % 2) for i in range(n)]
    swap_side = [(i, i ^ 1) for i in range(n)]
    from_line = lax.ppermute(tail_line, "rows", swap_line)
    from_side = lax.ppermute(tail_side, "rows", swap_side)
    ready_gate, ready_up, column_gate, column_up = write_out(n, ready_gate, ready_up, column_gate, column_up)
    ready_up = place_tails(n, ready_up, from_line, from_side)
    return ready_gate, ready_up, column_gate, column_up


def solution(mesh):
    split = P("rows", "width")
    return jax.shard_map(
        functools.partial(per_device, mesh.shape["rows"]),
        mesh=mesh,
        in_specs=(split,) * 6 + (P("rows"),),
        out_specs=(P(None, "width"), P(None, "width"), P("width"), P("width")),
        check_vma=False,
    )
```

```python
import functools

import jax
import jax.numpy as jnp
from jax import lax
from jax.experimental import pallas as pl
from jax.experimental.pallas import tpu as pltpu
from jax.sharding import PartitionSpec as P

learn_rate = 0.02
decay_rate = 0.1
tiny_value = 1e-08
lanes = 128
vmem_bytes = 67043328
block_rows = 16
MESH = pl.DeviceIdType.MESH
scope = jax.named_scope


def column_chunks(columns):
    tiles = columns // lanes
    first, second, last = max(1, tiles // 9), max(1, (tiles + 1) // 4), max(1, tiles * 3 // 8)
    gate = [first, second] + even(tiles - first - second, 2)
    up = even(tiles - last, 3) + [last]
    chunks = []
    for t, sizes, at in ((0, gate, 0), (1, up, last)):
        for size in sizes:
            if size:
                chunks.append((t, at % tiles * lanes, size * lanes))
            at += size
    return chunks


def even(tiles, pieces):
    return [tiles // pieces + (1 if i < tiles % pieces else 0) for i in range(pieces)]


def gather_kernel(
    n, gain_ref, wg, mg, sg, wu, mu, su, out_gate, out_up, col_gate, col_up, tail_line, tail_side,
    held, gain_row, gain_wide, parts, raw,
    gain_sem, in_sem, part_send, part_recv, send_sem, line_recv, mate_recv, rest_recv, tail_sem, raw_send, raw_recv,
):
    me = lax.axis_index("rows")
    w = lax.axis_index("width")
    length = n // 2
    place, side = me // 2, me % 2
    mate = place + 1 - 2 * (place % 2)
    lead = w % 2 == 1
    far = jnp.where(place * 2 < length, length - 1, 0)
    rows, columns = wg.shape
    chunks = column_chunks(columns)
    half = sum(t == 0 for t, _, _ in chunks)
    last = len(chunks) - 1
    start, tail = chunks[0][2], chunks[last][2]
    sources = ((wg, mg, sg), (wu, mu, su))
    outs = (out_gate, out_up)
    cols = (col_gate, col_up)

    barrier = pltpu.get_barrier_semaphore()

    def greet(i, carry):
        peer = lax.rem(me + i, n)
        pl.semaphore_signal(barrier, inc=1, device_id=(peer, w), device_id_type=MESH)
        return carry

    lax.fori_loop(1, n, greet, 0)

    def fetch(k):
        t, at, size = chunks[k]
        for i, src in enumerate(sources[t]):
            pltpu.make_async_copy(
                src.at[:, pl.ds(at, size)], held.at[i, t, :, pl.ds(at, size)], in_sem.at[k]
            ).start()

    def fetched(k):
        t, at, size = chunks[k]
        here = held.at[:, t, :, pl.ds(at, size)]
        pltpu.make_async_copy(here, here, in_sem.at[k]).wait()

    gain_copy = pltpu.make_async_copy(gain_ref, gain_row.at[0], gain_sem)
    gain_copy.start()
    fetch(0)
    fetch(1)
    with scope("gain"):
        gain_copy.wait()
    for r in range(0, rows, 8):
        at = r // lanes * lanes
        wide = min(lanes, rows - at)
        row = jnp.broadcast_to(gain_row[:, pl.ds(at, wide)], (8, wide))
        lane = lax.broadcasted_iota(jnp.int32, (8, wide), 1)
        here = lax.broadcasted_iota(jnp.int32, (8, wide), 0) + (r - at)
        picked = jnp.sum(jnp.where(lane == here, row, 0.0), axis=1, keepdims=True)
        gain_wide[pl.ds(r, 8), :] = jnp.broadcast_to(picked, (8, lanes))

    groups = [[0, 1], list(range(2, half)), list(range(half, len(chunks)))]

    def span(g):
        t = chunks[groups[g][0]][0]
        return t, min(chunks[k][1] for k in groups[g]), sum(chunks[k][2] for k in groups[g])

    def part_copy(g, peer):
        t, at, size = span(g)
        here = parts.at[me, t, :, pl.ds(at, size)]
        return pltpu.make_async_remote_copy(
            src_ref=here, dst_ref=here, send_sem=part_send, recv_sem=part_recv.at[g],
            device_id=(peer, w), device_id_type=MESH,
        )

    def compute(k):
        t, at, size = chunks[k]
        with scope(f"fetched{k}"):
            fetched(k)

        def step(b, total):
            here = pl.ds(pl.multiple_of(b * block_rows, block_rows), block_rows)
            there = pl.ds(at, size)
            weight = held[0, t, here, there]
            latest = weight - learn_rate * (
                held[1, t, here, there] / (jnp.sqrt(held[2, t, here, there]) + tiny_value) + decay_rate * weight
            )
            gain = jnp.concatenate([gain_wide[here, :]] * (size // lanes), axis=1)
            gained = latest * gain
            held[0, t, here, there] = gained
            squared = gained * gained
            for r in range(0, block_rows, 8):
                total = total + squared[r : r + 8]
            return total

        total = lax.fori_loop(0, rows // block_rows, step, jnp.zeros((8, size), jnp.float32))
        parts[me, t, :, pl.ds(at, size)] = jnp.sum(total, axis=0, keepdims=True)

    def share_parts(g):
        def send(i, carry):
            part_copy(g, lax.rem(me + i, n)).start()
            return carry

        lax.fori_loop(1, n, send, 0)

    def parts_arrived(g):
        t, at, size = span(g)
        refs = parts.at[pl.ds(0, n - 1), t, :, pl.ds(at, size)]
        pltpu.make_async_copy(refs, refs, part_recv.at[g]).wait()

    def block(share, k):
        t, at, size = chunks[k]
        start = pl.multiple_of(share * rows, rows)
        return outs[t].at[pl.ds(start, rows), pl.ds(at, size)]

    def push(link, share, k, recv, send):
        there = ((place - 1) * 2 + side, (place + 1) * 2 + side, place * 2 + 1 - side)[link]
        here = block(share, k)
        pltpu.make_async_remote_copy(
            src_ref=here, dst_ref=here, send_sem=send_sem.at[send], recv_sem=recv,
            device_id=(there, w), device_id_type=MESH,
        ).start()

    def arrived(share, k, recv):
        here = block(share, k)
        pltpu.make_async_copy(here, here, recv).wait()

    def push_line(link, q, k):
        push(link, q * 2 + side, k, line_recv.at[q, k], 8 + link if k == 0 else link * 2 + chunks[k][0])

    def push_side(q, k, own=False):
        share = q * 2 + side
        if k == 0:
            push(2, share, k, rest_recv.at[4], 10)
        elif k < half:
            push(2, share, k, rest_recv.at[0], 4)
        elif own:
            push(2, share, k, mate_recv.at[k - half], 6 if k == last else 5)
        elif k < last:
            @pl.when(q != mate)
            def _():
                push(2, share, k, rest_recv.at[1], 5)
        else:
            @pl.when((q != mate) & (q != far))
            def _():
                push(2, share, k, rest_recv.at[3], 6)

    def raw_copy(link):
        t, at, size = chunks[0]
        there = ((place - 1) * 2 + side, (place + 1) * 2 + side, place * 2 + 1 - side)[link]
        return pltpu.make_async_remote_copy(
            src_ref=held.at[0, t, :, pl.ds(at, size)], dst_ref=raw.at[link],
            send_sem=raw_send.at[link], recv_sem=raw_recv.at[link],
            device_id=(there, w), device_id_type=MESH,
        )

    def each_raw(action):
        @pl.when(place > 0)
        def _():
            action(raw_copy(0))

        @pl.when(place < length - 1)
        def _():
            action(raw_copy(1))

        action(raw_copy(2))

    def take_raw(link, share):
        t, at, size = chunks[0]
        pltpu.make_async_copy(raw.at[link], raw.at[link], raw_recv.at[link]).wait()
        scale = cols[t][:, pl.ds(at, size)]

        def step(b, carry):
            here = pl.ds(pl.multiple_of(b * block_rows, block_rows), block_rows)
            there = pl.ds(pl.multiple_of(share * rows + b * block_rows, block_rows), block_rows)
            outs[t][there, pl.ds(at, size)] = (raw[link, here, :] / scale).astype(jnp.bfloat16)
            return carry

        lax.fori_loop(0, rows // block_rows, step, 0)

    def line_arrived(q, k, d, link):
        if k == 0:
            @pl.when(lead & (d == 1))
            def _():
                take_raw(link, q * 2 + side)

            @pl.when(jnp.logical_not(lead & (d == 1)))
            def _():
                arrived(q * 2 + side, k, line_recv.at[q, k])
        else:
            arrived(q * 2 + side, k, line_recv.at[q, k])

    def finish(k):
        t, at, size = chunks[k]
        for g, group in enumerate(groups):
            if k == (1 if g == 0 else group[0]):
                with scope(f"parts{g}"):
                    parts_arrived(g)
        total = parts[0, t, :, pl.ds(at, size)]
        for i in range(1, n):
            total = total + parts[i, t, :, pl.ds(at, size)]
        scale = jnp.sqrt(total)
        cols[t][:, pl.ds(at, size)] = scale

        def step(b, carry):
            here = pl.ds(pl.multiple_of(b * block_rows, block_rows), block_rows)
            there = pl.ds(pl.multiple_of(me * rows + b * block_rows, block_rows), block_rows)
            outs[t][there, pl.ds(at, size)] = (held[0, t, here, pl.ds(at, size)] / scale).astype(jnp.bfloat16)
            return carry

        lax.fori_loop(0, rows // block_rows, step, 0)

    def send_own(k):
        @pl.when(place > 0)
        def _():
            push_line(0, place, k)

        @pl.when(place < length - 1)
        def _():
            push_line(1, place, k)

        push_side(place, k, own=True)

    for k in range(2, len(chunks)):
        fetch(k)
    compute(0)
    compute(1)
    with scope("barrier"):
        pl.semaphore_wait(barrier, n - 1)

    @pl.when(lead)
    def _():
        share_parts(0)
        each_raw(lambda copy: copy.start())

    for k in groups[1]:
        compute(k)

    @pl.when(jnp.logical_not(lead))
    def _():
        share_parts(0)

    share_parts(1)
    for k in [1, 0] + list(range(2, len(chunks))):
        finish(k)
        with scope(f"own{k}"):
            if k == 0:
                @pl.when(jnp.logical_not(lead))
                def _():
                    send_own(k)
            else:
                send_own(k)
        if k == 0:
            for i in groups[2]:
                compute(i)
            share_parts(2)

    def spread(d, carry):
        for k in range(len(chunks)):
            @pl.when(place + d < length)
            def _():
                q = place + d
                with scope(f"R{k}"):
                    line_arrived(q, k, d, 0)

                @pl.when(place > 0)
                def _():
                    push_line(0, q, k)

                push_side(q, k)

            @pl.when(place - d >= 0)
            def _():
                q = place - d
                with scope(f"L{k}"):
                    line_arrived(q, k, d, 1)

                @pl.when(place < length - 1)
                def _():
                    push_line(1, q, k)

                push_side(q, k)

        return carry

    middle = max(1, length // 2) + 1
    lax.fori_loop(1, middle, spread, 0)

    other = place * 2 + 1 - side
    for k in range(half, len(chunks)):
        with scope(f"X{k}"):
            arrived(other, k, mate_recv.at[k - half])
        if k < last:
            @pl.when(mate < place)
            def _():
                push(0, other, k, rest_recv.at[2], 7)

            @pl.when(mate > place)
            def _():
                push(1, other, k, rest_recv.at[2], 7)

    line_copy = pltpu.make_async_copy(block(other, last), tail_line, tail_sem.at[0])
    line_copy.start()
    lax.fori_loop(middle, length, spread, 0)
    side_copy = pltpu.make_async_copy(block(far * 2 + side, last), tail_side, tail_sem.at[1])
    side_copy.start()

    def pass_bytes(t, shares, sem, at=0, size=columns):
        here = outs[t].at[pl.ds(0, shares * rows), pl.ds(at, size)]
        pltpu.make_async_copy(here, here, sem).wait()

    with scope("rest"):
        pass_bytes(0, length, rest_recv.at[0], start, columns - start)

        @pl.when(lead)
        def _():
            pass_bytes(0, length - 1, rest_recv.at[4], 0, start)
            take_raw(2, other)

        @pl.when(jnp.logical_not(lead))
        def _():
            pass_bytes(0, length, rest_recv.at[4], 0, start)

        pass_bytes(1, length - 2, rest_recv.at[1], tail, columns - tail)
        pass_bytes(1, 1, rest_recv.at[2], tail, columns - tail)
        pass_bytes(1, length - 3, rest_recv.at[3], 0, tail)

    with scope("drain"):
        everyone = parts.at[pl.ds(0, n - 1)]
        pltpu.make_async_copy(everyone, everyone, part_send).wait()
        pass_bytes(0, length, send_sem.at[4], start, columns - start)
        pass_bytes(1, length - 1, send_sem.at[5], tail, columns - tail)
        pass_bytes(1, length - 2, send_sem.at[6], 0, tail)
        pass_bytes(1, 1, send_sem.at[7], tail, columns - tail)
        for p in range(length):
            @pl.when(place == p)
            def _():
                for link, shares in ((0, length - p), (1, p + 1)):
                    if (p, link) not in ((0, 0), (length - 1, 1)):
                        pass_bytes(0, shares, send_sem.at[link * 2], start, columns - start)
                        pass_bytes(1, shares, send_sem.at[link * 2 + 1])

        def first_sent(own):
            pass_bytes(0, length - 1 + own, send_sem.at[10], 0, start)
            for p in range(length):
                @pl.when(place == p)
                def _():
                    for link, shares in ((0, length - p - 1 + own), (1, p + own)):
                        if shares and (p, link) not in ((0, 0), (length - 1, 1)):
                            pass_bytes(0, shares, send_sem.at[8 + link], 0, start)

        @pl.when(lead)
        def _():
            first_sent(0)
            each_raw(lambda copy: copy.wait_send())

        @pl.when(jnp.logical_not(lead))
        def _():
            first_sent(1)

        line_copy.wait()
        side_copy.wait()


def write_kernel(pieces, gate, up, col_gate, col_up, out_gate, out_up, out_col_gate, out_col_up, sem):
    step = gate.shape[0] // pieces
    for i in range(pieces):
        for t, (src, dst) in enumerate(((gate, out_gate), (up, out_up))):
            pltpu.make_async_copy(src.at[pl.ds(i * step, step)], dst.at[pl.ds(i * step, step)], sem.at[t]).start()
    small = [
        pltpu.make_async_copy(src.at[0], dst, sem.at[2 + t])
        for t, (src, dst) in enumerate(((col_gate, out_col_gate), (col_up, out_col_up)))
    ]
    for copy in small:
        copy.start()
    for t, (src, dst) in enumerate(((gate, out_gate), (up, out_up))):
        pltpu.make_async_copy(src, dst, sem.at[t]).wait()
    for copy in small:
        copy.wait()


def write_out(pieces, gate, up, col_gate, col_up):
    vmem = pl.BlockSpec(memory_space=pltpu.VMEM)
    hbm = pl.BlockSpec(memory_space=pltpu.HBM)
    flat = jax.ShapeDtypeStruct((col_gate.shape[1],), col_gate.dtype)
    return pl.pallas_call(
        functools.partial(write_kernel, pieces),
        out_shape=[jax.ShapeDtypeStruct(a.shape, a.dtype) for a in (gate, up)] + [flat, flat],
        in_specs=[vmem] * 4,
        out_specs=[hbm] * 4,
        scratch_shapes=[pltpu.SemaphoreType.DMA((4,))],
        compiler_params=pltpu.CompilerParams(vmem_limit_bytes=2**20),
        cost_estimate=pl.CostEstimate(flops=10**8, bytes_accessed=4 * gate.size, transcendentals=0),
        name="write_out",
    )(gate, up, col_gate, col_up)


def place_kernel(n, up, from_line, from_side, out, sem):
    me = lax.axis_index("rows")
    place, side = me // 2, me % 2
    mate = place + 1 - 2 * (place % 2)
    far = jnp.where(place * 2 < n // 2, n // 2 - 1, 0)
    rows, tail = from_line.shape
    copies = []
    for i, (src, q) in enumerate(((from_line, mate), (from_side, far))):
        start = pl.multiple_of((q * 2 + 1 - side) * rows, rows)
        there = out.at[pl.ds(start, rows), pl.ds(0, tail)]
        copies.append(pltpu.make_async_copy(src, there, sem.at[i]))
    for copy in copies:
        copy.start()
    for copy in copies:
        copy.wait()


def place_tails(n, up, from_line, from_side):
    vmem = pl.BlockSpec(memory_space=pltpu.VMEM)
    hbm = pl.BlockSpec(memory_space=pltpu.HBM)
    return pl.pallas_call(
        functools.partial(place_kernel, n),
        out_shape=jax.ShapeDtypeStruct(up.shape, up.dtype),
        in_specs=[hbm, vmem, vmem],
        out_specs=hbm,
        input_output_aliases={0: 0},
        scratch_shapes=[pltpu.SemaphoreType.DMA((2,))],
        compiler_params=pltpu.CompilerParams(vmem_limit_bytes=2**22),
        name="place_tails",
    )(up, from_line, from_side)


def per_device(n, weight_gate, moment_gate, square_gate, weight_up, moment_up, square_up, norm_gain):
    rows, columns = weight_gate.shape
    length = n // 2
    chunks = column_chunks(columns)
    count, tail = len(chunks), chunks[-1][2]
    up_count = sum(t for t, _, _ in chunks)
    vmem = pl.BlockSpec(memory_space=pltpu.VMEM)
    hbm = pl.BlockSpec(memory_space=pltpu.HBM)
    room = vmem_bytes - 2 * n * rows * columns * 2 - 3 * 2**19
    ready_gate, ready_up, column_gate, column_up, tail_line, tail_side = pl.pallas_call(
        functools.partial(gather_kernel, n),
        out_shape=(
            pltpu.VMEM((n * rows, columns), jnp.bfloat16),
            pltpu.VMEM((n * rows, columns), jnp.bfloat16),
            pltpu.VMEM((1, columns), jnp.float32),
            pltpu.VMEM((1, columns), jnp.float32),
            jax.ShapeDtypeStruct((rows, tail), jnp.bfloat16),
            jax.ShapeDtypeStruct((rows, tail), jnp.bfloat16),
        ),
        in_specs=[hbm] * 7,
        out_specs=(vmem, vmem, vmem, vmem, hbm, hbm),
        scratch_shapes=[
            pltpu.VMEM((3, 2, rows, columns), jnp.float32),
            pltpu.VMEM((1, rows), jnp.float32),
            pltpu.VMEM((rows, lanes), jnp.float32),
            pltpu.VMEM((n, 2, 1, columns), jnp.float32),
            pltpu.VMEM((3, rows, chunks[0][2]), jnp.float32),
            pltpu.SemaphoreType.DMA,
            pltpu.SemaphoreType.DMA((count,)),
            pltpu.SemaphoreType.DMA,
            pltpu.SemaphoreType.DMA((3,)),
            pltpu.SemaphoreType.DMA((11,)),
            pltpu.SemaphoreType.DMA((length, count)),
            pltpu.SemaphoreType.DMA((up_count,)),
            pltpu.SemaphoreType.DMA((5,)),
            pltpu.SemaphoreType.DMA((2,)),
            pltpu.SemaphoreType.DMA((3,)),
            pltpu.SemaphoreType.DMA((3,)),
        ],
        compiler_params=pltpu.CompilerParams(
            collective_id=0, has_side_effects=True, vmem_limit_bytes=room
        ),
        name="step_and_gather",
    )(norm_gain, weight_gate, moment_gate, square_gate, weight_up, moment_up, square_up)
    swap_line = [(i, (i // 2 ^ 1) * 2 + i % 2) for i in range(n)]
    swap_side = [(i, i ^ 1) for i in range(n)]
    from_line = lax.ppermute(tail_line, "rows", swap_line)
    from_side = lax.ppermute(tail_side, "rows", swap_side)
    ready_gate, ready_up, column_gate, column_up = write_out(n, ready_gate, ready_up, column_gate, column_up)
    ready_up = place_tails(n, ready_up, from_line, from_side)
    return ready_gate, ready_up, column_gate, column_up


def solution(mesh):
    split = P("rows", "width")
    return jax.shard_map(
        functools.partial(per_device, mesh.shape["rows"]),
        mesh=mesh,
        in_specs=(split,) * 6 + (P("rows"),),
        out_specs=(P(None, "width"), P(None, "width"), P("width"), P("width")),
        check_vma=False,
    )
```

```python
import functools

import jax
import jax.numpy as jnp
from jax import lax
from jax.experimental import pallas as pl
from jax.experimental.pallas import tpu as pltpu
from jax.sharding import PartitionSpec as P

learn_rate = 0.02
decay_rate = 0.1
tiny_value = 1e-08
lanes = 128
vmem_bytes = 67043328
block_rows = 16
MESH = pl.DeviceIdType.MESH
scope = jax.named_scope


def column_chunks(columns):
    tiles = columns // lanes
    first, second, last = max(1, tiles // 9), max(1, tiles // 4), max(1, tiles * 3 // 8)
    gate = [first, second] + even(tiles - first - second, 2)
    up = even(tiles - last, 3) + [last]
    chunks = []
    for t, sizes, at in ((0, gate, 0), (1, up, last)):
        for size in sizes:
            if size:
                chunks.append((t, at % tiles * lanes, size * lanes))
            at += size
    return chunks


def even(tiles, pieces):
    return [tiles // pieces + (1 if i < tiles % pieces else 0) for i in range(pieces)]


def gather_kernel(
    n, gain_ref, wg, mg, sg, wu, mu, su, out_gate, out_up, col_gate, col_up, tail_line, tail_side,
    held, gain_row, gain_wide, parts, pairs, raw,
    gain_sem, in_sem, part_send, part_recv, pair_recv, send_sem, line_recv, mate_recv, rest_recv, tail_sem, raw_send, raw_recv,
):
    me = lax.axis_index("rows")
    w = lax.axis_index("width")
    length = n // 2
    place, side = me // 2, me % 2
    mate = place + 1 - 2 * (place % 2)
    lead = w % 2 == 1
    far = jnp.where(place * 2 < length, length - 1, 0)
    rows, columns = wg.shape
    chunks = column_chunks(columns)
    half = sum(t == 0 for t, _, _ in chunks)
    last = len(chunks) - 1
    start, tail = chunks[0][2], chunks[last][2]
    sources = ((wg, mg, sg), (wu, mu, su))
    outs = (out_gate, out_up)
    cols = (col_gate, col_up)

    barrier = pltpu.get_barrier_semaphore()

    def greet(i, carry):
        peer = lax.rem(me + i, n)
        pl.semaphore_signal(barrier, inc=1, device_id=(peer, w), device_id_type=MESH)
        return carry

    lax.fori_loop(1, n, greet, 0)

    def fetch(k):
        t, at, size = chunks[k]
        for i, src in enumerate(sources[t]):
            pltpu.make_async_copy(
                src.at[:, pl.ds(at, size)], held.at[i, t, :, pl.ds(at, size)], in_sem.at[k]
            ).start()

    def fetched(k):
        t, at, size = chunks[k]
        here = held.at[:, t, :, pl.ds(at, size)]
        pltpu.make_async_copy(here, here, in_sem.at[k]).wait()

    gain_copy = pltpu.make_async_copy(gain_ref, gain_row.at[0], gain_sem)
    gain_copy.start()
    fetch(0)
    fetch(1)
    with scope("gain"):
        gain_copy.wait()
    for r in range(0, rows, 8):
        at = r // lanes * lanes
        wide = min(lanes, rows - at)
        row = jnp.broadcast_to(gain_row[:, pl.ds(at, wide)], (8, wide))
        lane = lax.broadcasted_iota(jnp.int32, (8, wide), 1)
        here = lax.broadcasted_iota(jnp.int32, (8, wide), 0) + (r - at)
        picked = jnp.sum(jnp.where(lane == here, row, 0.0), axis=1, keepdims=True)
        gain_wide[pl.ds(r, 8), :] = jnp.broadcast_to(picked, (8, lanes))

    groups = [[0, 1], list(range(2, half)), list(range(half, len(chunks)))]

    def span(g):
        t = chunks[groups[g][0]][0]
        return t, min(chunks[k][1] for k in groups[g]), sum(chunks[k][2] for k in groups[g])

    def part_copy(g, source, slot, peer, recv):
        t, at, size = span(g)
        here = source.at[slot, t, :, pl.ds(at, size)]
        return pltpu.make_async_remote_copy(
            src_ref=here, dst_ref=here, send_sem=part_send.at[t], recv_sem=recv.at[g],
            device_id=(peer, w), device_id_type=MESH,
        )

    def compute(k):
        t, at, size = chunks[k]
        with scope(f"fetched{k}"):
            fetched(k)

        def step(b, total):
            here = pl.ds(pl.multiple_of(b * block_rows, block_rows), block_rows)
            there = pl.ds(at, size)
            weight = held[0, t, here, there]
            latest = weight - learn_rate * (
                held[1, t, here, there] / (jnp.sqrt(held[2, t, here, there]) + tiny_value) + decay_rate * weight
            )
            gain = jnp.concatenate([gain_wide[here, :]] * (size // lanes), axis=1)
            gained = latest * gain
            held[0, t, here, there] = gained
            squared = gained * gained
            for r in range(0, block_rows, 8):
                total = total + squared[r : r + 8]
            return total

        total = lax.fori_loop(0, rows // block_rows, step, jnp.zeros((8, size), jnp.float32))
        parts[me, t, :, pl.ds(at, size)] = jnp.sum(total, axis=0, keepdims=True)

    def share_parts(g):
        def send(i, carry):
            part_copy(g, parts, me, lax.rem(me + i, n), part_recv).start()
            return carry

        lax.fori_loop(1, n, send, 0)

    def share_pair(g):
        part_copy(g, parts, me, place * 2 + 1 - side, pair_recv).start()

    def share_line(g):
        t, at, size = span(g)
        there = pl.ds(at, size)
        one = parts.at[0, t, :, there]
        pltpu.make_async_copy(one, one, pair_recv.at[g]).wait()
        pairs[place, t, :, there] = parts[me, t, :, there] + parts[place * 2 + 1 - side, t, :, there]

        def send(i, carry):
            part_copy(g, pairs, place, lax.rem(place + i, length) * 2 + side, part_recv).start()
            return carry

        lax.fori_loop(1, length, send, 0)

    def gather_parts(g, source, count):
        t, at, size = span(g)
        there = pl.ds(at, size)
        refs = source.at[pl.ds(0, count - 1), t, :, there]
        pltpu.make_async_copy(refs, refs, part_recv.at[g]).wait()
        total = source[0, t, :, there]
        for i in range(1, count):
            total = total + source[i, t, :, there]
        cols[t][:, there] = jnp.sqrt(total)

    def parts_arrived(g):
        if g == 2:
            gather_parts(g, pairs, length)
        else:
            @pl.when(lead)
            def _():
                gather_parts(g, parts, n)

            @pl.when(jnp.logical_not(lead))
            def _():
                gather_parts(g, pairs, length)

    def block(share, k):
        t, at, size = chunks[k]
        start = pl.multiple_of(share * rows, rows)
        return outs[t].at[pl.ds(start, rows), pl.ds(at, size)]

    def push(link, share, k, recv, send):
        there = ((place - 1) * 2 + side, (place + 1) * 2 + side, place * 2 + 1 - side)[link]
        here = block(share, k)
        pltpu.make_async_remote_copy(
            src_ref=here, dst_ref=here, send_sem=send_sem.at[send], recv_sem=recv,
            device_id=(there, w), device_id_type=MESH,
        ).start()

    def arrived(share, k, recv):
        here = block(share, k)
        pltpu.make_async_copy(here, here, recv).wait()

    def push_line(link, q, k):
        push(link, q * 2 + side, k, line_recv.at[q, k], 8 + link if k == 0 else link * 2 + chunks[k][0])

    def push_side(q, k, own=False):
        share = q * 2 + side
        if k == 0:
            push(2, share, k, rest_recv.at[4], 10)
        elif k < half:
            push(2, share, k, rest_recv.at[0], 4)
        elif own:
            push(2, share, k, mate_recv.at[k - half], 6 if k == last else 5)
        elif k < last:
            @pl.when(q != mate)
            def _():
                push(2, share, k, rest_recv.at[1], 5)
        else:
            @pl.when((q != mate) & (q != far))
            def _():
                push(2, share, k, rest_recv.at[3], 6)

    def raw_copy(link):
        t, at, size = chunks[0]
        there = ((place - 1) * 2 + side, (place + 1) * 2 + side, place * 2 + 1 - side)[link]
        return pltpu.make_async_remote_copy(
            src_ref=held.at[0, t, :, pl.ds(at, size)], dst_ref=raw.at[link],
            send_sem=raw_send.at[link], recv_sem=raw_recv.at[link],
            device_id=(there, w), device_id_type=MESH,
        )

    def each_raw(action):
        @pl.when(place > 0)
        def _():
            action(raw_copy(0))

        @pl.when(place < length - 1)
        def _():
            action(raw_copy(1))

        action(raw_copy(2))

    def take_raw(link, share):
        t, at, size = chunks[0]
        pltpu.make_async_copy(raw.at[link], raw.at[link], raw_recv.at[link]).wait()
        scale = cols[t][:, pl.ds(at, size)]

        def step(b, carry):
            here = pl.ds(pl.multiple_of(b * block_rows, block_rows), block_rows)
            there = pl.ds(pl.multiple_of(share * rows + b * block_rows, block_rows), block_rows)
            outs[t][there, pl.ds(at, size)] = (raw[link, here, :] / scale).astype(jnp.bfloat16)
            return carry

        lax.fori_loop(0, rows // block_rows, step, 0)

    def line_arrived(q, k, d, link):
        if k == 0:
            @pl.when(lead & (d == 1))
            def _():
                take_raw(link, q * 2 + side)

            @pl.when(jnp.logical_not(lead & (d == 1)))
            def _():
                arrived(q * 2 + side, k, line_recv.at[q, k])
        else:
            arrived(q * 2 + side, k, line_recv.at[q, k])

    def finish(k):
        t, at, size = chunks[k]
        for g, group in enumerate(groups):
            if k == (1 if g == 0 else group[0]):
                with scope(f"parts{g}"):
                    parts_arrived(g)
        scale = cols[t][:, pl.ds(at, size)]

        def step(b, carry):
            here = pl.ds(pl.multiple_of(b * block_rows, block_rows), block_rows)
            there = pl.ds(pl.multiple_of(me * rows + b * block_rows, block_rows), block_rows)
            outs[t][there, pl.ds(at, size)] = (held[0, t, here, pl.ds(at, size)] / scale).astype(jnp.bfloat16)
            return carry

        lax.fori_loop(0, rows // block_rows, step, 0)

    def send_own(k):
        @pl.when(place > 0)
        def _():
            push_line(0, place, k)

        @pl.when(place < length - 1)
        def _():
            push_line(1, place, k)

        push_side(place, k, own=True)

    for k in range(2, len(chunks)):
        fetch(k)
    compute(0)
    compute(1)
    with scope("barrier"):
        pl.semaphore_wait(barrier, n - 1)

    @pl.when(lead)
    def _():
        share_parts(0)
        each_raw(lambda copy: copy.start())

    @pl.when(jnp.logical_not(lead))
    def _():
        share_pair(0)

    for k in groups[1]:
        compute(k)

    @pl.when(lead)
    def _():
        share_parts(1)

    @pl.when(jnp.logical_not(lead))
    def _():
        share_pair(1)
        with scope("line"):
            share_line(0)
        for i in groups[2]:
            compute(i)
        share_pair(2)
        share_line(1)

    for k in [1, 0] + list(range(2, len(chunks))):
        if k == groups[1][-1]:
            with scope("line2"):
                share_line(2)
        finish(k)
        with scope(f"own{k}"):
            if k == 0:
                @pl.when(jnp.logical_not(lead))
                def _():
                    send_own(k)
            else:
                send_own(k)
        if k == 0:
            @pl.when(lead)
            def _():
                for i in groups[2]:
                    compute(i)
                share_pair(2)

    def spread(d, carry):
        for k in range(len(chunks)):
            @pl.when(place + d < length)
            def _():
                q = place + d
                with scope(f"R{k}"):
                    line_arrived(q, k, d, 0)

                @pl.when(place > 0)
                def _():
                    push_line(0, q, k)

                push_side(q, k)

            @pl.when(place - d >= 0)
            def _():
                q = place - d
                with scope(f"L{k}"):
                    line_arrived(q, k, d, 1)

                @pl.when(place < length - 1)
                def _():
                    push_line(1, q, k)

                push_side(q, k)

        return carry

    middle = max(1, length // 2) + 1
    lax.fori_loop(1, middle, spread, 0)

    other = place * 2 + 1 - side
    for k in range(half, len(chunks)):
        with scope(f"X{k}"):
            arrived(other, k, mate_recv.at[k - half])
        if k < last:
            @pl.when(mate < place)
            def _():
                push(0, other, k, rest_recv.at[2], 7)

            @pl.when(mate > place)
            def _():
                push(1, other, k, rest_recv.at[2], 7)

    line_copy = pltpu.make_async_copy(block(other, last), tail_line, tail_sem.at[0])
    line_copy.start()
    lax.fori_loop(middle, length, spread, 0)
    side_copy = pltpu.make_async_copy(block(far * 2 + side, last), tail_side, tail_sem.at[1])
    side_copy.start()

    def pass_bytes(t, shares, sem, at=0, size=columns):
        here = outs[t].at[pl.ds(0, shares * rows), pl.ds(at, size)]
        pltpu.make_async_copy(here, here, sem).wait()

    with scope("rest"):
        pass_bytes(0, length, rest_recv.at[0], start, columns - start)

        @pl.when(lead)
        def _():
            pass_bytes(0, length - 1, rest_recv.at[4], 0, start)
            take_raw(2, other)

        @pl.when(jnp.logical_not(lead))
        def _():
            pass_bytes(0, length, rest_recv.at[4], 0, start)

        pass_bytes(1, length - 2, rest_recv.at[1], tail, columns - tail)
        pass_bytes(1, 1, rest_recv.at[2], tail, columns - tail)
        pass_bytes(1, length - 3, rest_recv.at[3], 0, tail)

    with scope("drain"):
        def parts_sent(t, count):
            sent = parts.at[pl.ds(0, count), t]
            pltpu.make_async_copy(sent, sent, part_send.at[t]).wait()

        parts_sent(1, length)

        @pl.when(lead)
        def _():
            parts_sent(0, n - 1)

        @pl.when(jnp.logical_not(lead))
        def _():
            parts_sent(0, length)

        pass_bytes(0, length, send_sem.at[4], start, columns - start)
        pass_bytes(1, length - 1, send_sem.at[5], tail, columns - tail)
        pass_bytes(1, length - 2, send_sem.at[6], 0, tail)
        pass_bytes(1, 1, send_sem.at[7], tail, columns - tail)
        for p in range(length):
            @pl.when(place == p)
            def _():
                for link, shares in ((0, length - p), (1, p + 1)):
                    if (p, link) not in ((0, 0), (length - 1, 1)):
                        pass_bytes(0, shares, send_sem.at[link * 2], start, columns - start)
                        pass_bytes(1, shares, send_sem.at[link * 2 + 1])

        def first_sent(own):
            pass_bytes(0, length - 1 + own, send_sem.at[10], 0, start)
            for p in range(length):
                @pl.when(place == p)
                def _():
                    for link, shares in ((0, length - p - 1 + own), (1, p + own)):
                        if shares and (p, link) not in ((0, 0), (length - 1, 1)):
                            pass_bytes(0, shares, send_sem.at[8 + link], 0, start)

        @pl.when(lead)
        def _():
            first_sent(0)
            each_raw(lambda copy: copy.wait_send())

        @pl.when(jnp.logical_not(lead))
        def _():
            first_sent(1)

        line_copy.wait()
        side_copy.wait()


def write_kernel(pieces, gate, up, col_gate, col_up, out_gate, out_up, out_col_gate, out_col_up, sem):
    step = gate.shape[0] // pieces
    for i in range(pieces):
        for t, (src, dst) in enumerate(((gate, out_gate), (up, out_up))):
            pltpu.make_async_copy(src.at[pl.ds(i * step, step)], dst.at[pl.ds(i * step, step)], sem.at[t]).start()
    small = [
        pltpu.make_async_copy(src.at[0], dst, sem.at[2 + t])
        for t, (src, dst) in enumerate(((col_gate, out_col_gate), (col_up, out_col_up)))
    ]
    for copy in small:
        copy.start()
    for t, (src, dst) in enumerate(((gate, out_gate), (up, out_up))):
        pltpu.make_async_copy(src, dst, sem.at[t]).wait()
    for copy in small:
        copy.wait()


def write_out(pieces, gate, up, col_gate, col_up):
    vmem = pl.BlockSpec(memory_space=pltpu.VMEM)
    hbm = pl.BlockSpec(memory_space=pltpu.HBM)
    flat = jax.ShapeDtypeStruct((col_gate.shape[1],), col_gate.dtype)
    return pl.pallas_call(
        functools.partial(write_kernel, pieces),
        out_shape=[jax.ShapeDtypeStruct(a.shape, a.dtype) for a in (gate, up)] + [flat, flat],
        in_specs=[vmem] * 4,
        out_specs=[hbm] * 4,
        scratch_shapes=[pltpu.SemaphoreType.DMA((4,))],
        compiler_params=pltpu.CompilerParams(vmem_limit_bytes=2**20),
        cost_estimate=pl.CostEstimate(flops=10**8, bytes_accessed=4 * gate.size, transcendentals=0),
        name="write_out",
    )(gate, up, col_gate, col_up)


def place_kernel(n, up, from_line, from_side, out, sem):
    me = lax.axis_index("rows")
    place, side = me // 2, me % 2
    mate = place + 1 - 2 * (place % 2)
    far = jnp.where(place * 2 < n // 2, n // 2 - 1, 0)
    rows, tail = from_line.shape
    copies = []
    for i, (src, q) in enumerate(((from_line, mate), (from_side, far))):
        start = pl.multiple_of((q * 2 + 1 - side) * rows, rows)
        there = out.at[pl.ds(start, rows), pl.ds(0, tail)]
        copies.append(pltpu.make_async_copy(src, there, sem.at[i]))
    for copy in copies:
        copy.start()
    for copy in copies:
        copy.wait()


def place_tails(n, up, from_line, from_side):
    vmem = pl.BlockSpec(memory_space=pltpu.VMEM)
    hbm = pl.BlockSpec(memory_space=pltpu.HBM)
    return pl.pallas_call(
        functools.partial(place_kernel, n),
        out_shape=jax.ShapeDtypeStruct(up.shape, up.dtype),
        in_specs=[hbm, vmem, vmem],
        out_specs=hbm,
        input_output_aliases={0: 0},
        scratch_shapes=[pltpu.SemaphoreType.DMA((2,))],
        compiler_params=pltpu.CompilerParams(vmem_limit_bytes=2**22),
        name="place_tails",
    )(up, from_line, from_side)


def per_device(n, weight_gate, moment_gate, square_gate, weight_up, moment_up, square_up, norm_gain):
    rows, columns = weight_gate.shape
    length = n // 2
    chunks = column_chunks(columns)
    count, tail = len(chunks), chunks[-1][2]
    up_count = sum(t for t, _, _ in chunks)
    vmem = pl.BlockSpec(memory_space=pltpu.VMEM)
    hbm = pl.BlockSpec(memory_space=pltpu.HBM)
    room = vmem_bytes - 2 * n * rows * columns * 2 - 3 * 2**19
    ready_gate, ready_up, column_gate, column_up, tail_line, tail_side = pl.pallas_call(
        functools.partial(gather_kernel, n),
        out_shape=(
            pltpu.VMEM((n * rows, columns), jnp.bfloat16),
            pltpu.VMEM((n * rows, columns), jnp.bfloat16),
            pltpu.VMEM((1, columns), jnp.float32),
            pltpu.VMEM((1, columns), jnp.float32),
            jax.ShapeDtypeStruct((rows, tail), jnp.bfloat16),
            jax.ShapeDtypeStruct((rows, tail), jnp.bfloat16),
        ),
        in_specs=[hbm] * 7,
        out_specs=(vmem, vmem, vmem, vmem, hbm, hbm),
        scratch_shapes=[
            pltpu.VMEM((3, 2, rows, columns), jnp.float32),
            pltpu.VMEM((1, rows), jnp.float32),
            pltpu.VMEM((rows, lanes), jnp.float32),
            pltpu.VMEM((n, 2, 1, columns), jnp.float32),
            pltpu.VMEM((length, 2, 1, columns), jnp.float32),
            pltpu.VMEM((3, rows, chunks[0][2]), jnp.float32),
            pltpu.SemaphoreType.DMA,
            pltpu.SemaphoreType.DMA((count,)),
            pltpu.SemaphoreType.DMA((2,)),
            pltpu.SemaphoreType.DMA((3,)),
            pltpu.SemaphoreType.DMA((3,)),
            pltpu.SemaphoreType.DMA((11,)),
            pltpu.SemaphoreType.DMA((length, count)),
            pltpu.SemaphoreType.DMA((up_count,)),
            pltpu.SemaphoreType.DMA((5,)),
            pltpu.SemaphoreType.DMA((2,)),
            pltpu.SemaphoreType.DMA((3,)),
            pltpu.SemaphoreType.DMA((3,)),
        ],
        compiler_params=pltpu.CompilerParams(
            collective_id=0, has_side_effects=True, vmem_limit_bytes=room
        ),
        name="step_and_gather",
    )(norm_gain, weight_gate, moment_gate, square_gate, weight_up, moment_up, square_up)
    swap_line = [(i, (i // 2 ^ 1) * 2 + i % 2) for i in range(n)]
    swap_side = [(i, i ^ 1) for i in range(n)]
    from_line = lax.ppermute(tail_line, "rows", swap_line)
    from_side = lax.ppermute(tail_side, "rows", swap_side)
    ready_gate, ready_up, column_gate, column_up = write_out(n, ready_gate, ready_up, column_gate, column_up)
    ready_up = place_tails(n, ready_up, from_line, from_side)
    return ready_gate, ready_up, column_gate, column_up


def solution(mesh):
    split = P("rows", "width")
    return jax.shard_map(
        functools.partial(per_device, mesh.shape["rows"]),
        mesh=mesh,
        in_specs=(split,) * 6 + (P("rows"),),
        out_specs=(P(None, "width"), P(None, "width"), P("width"), P("width")),
        check_vma=False,
    )
```
